32 devices in a mesh: gx: 4 (over y, core), gy: 4 (over z), gz: 2 (over x).
Axes of the slice: x: 2, y: 2, z: 4, core: 2. Of those that a mesh axis runs over, the one named last changes fastest.
Arguments:
- a_vals: float32 [4, 8, 2, 6, 128, 128], P('gy', 'gx', 'gz'), may hold values from -0.25 to 0.25
- a_cols: int32 [4, 8, 2, 6], P('gy', 'gx', 'gz'), may hold values from 0 to 15, as said below
- a_count: int32 [4, 8, 2], P('gy', 'gx', 'gz'), may hold values from 1 to 6, as said below
- p_vals: float32 [2, 16, 4, 1, 128, 128], P('gz', 'gy', 'gx'), may hold values from -6 to 6
- p_cols: int32 [2, 16, 4, 1], P('gz', 'gy', 'gx'), may hold values from 0 to 1, as said below
- p_count: int32 [2, 16, 4], P('gz', 'gy', 'gx'), may hold values from 0 to 1, as said below
Outputs:
- c_tiles: float32 [4096, 1024], P(('gy', 'gz'), 'gx')
The draws below stay inside these ranges and needn't reach their ends.
Inputs may be any that keep to these rules, and one draw needn't show every extreme that they name: `a_cols`: inner tile indices of one block row and slice are distinct across its 6 slots. Slots 0 to a_count - 1 are live; the block rows of every device include one with all 6 slots live. `p_cols`: column tiles of one block row and group are distinct across its 1 slots. Slots 0 to p_count - 1 are live; the block rows of every device include one with all 1 slots live.
All inputs are finite; a program needn't handle non-finite values.
Results may differ from the reference program's by a relative error of at most 0.0003.
Values sent between devices are 32-bit elements; how exact they have to be, the bound alone decides.
A program may use at most 128 MiB of HBM per device.

```python
import jax
import jax.numpy as jnp
from jax import lax

TILE = 128
ROWS_DEV = 2
SLOTS_A = 6
SLOTS_P = 1
COLS_DEV = 2
RX = 8
KZ = 16
N_GX = 4
N_GY = 4
N_GZ = 2


def draw_a_count(key, part):
    first = jax.random.randint(jax.random.fold_in(key, 11), (N_GY, RX, N_GZ), 1, SLOTS_A + 1)
    second = jax.random.randint(jax.random.fold_in(key, 12), (N_GY, RX, N_GZ), 1, SLOTS_A + 1)
    counts = jnp.minimum(first, second)
    picked = jax.random.randint(jax.random.fold_in(key, 13), (N_GY, RX // ROWS_DEV, 1, N_GZ), 0, ROWS_DEV)
    position = jnp.arange(ROWS_DEV, dtype=jnp.int32)[None, None, :, None]
    filled = (position == picked).reshape(N_GY, RX, N_GZ)
    return jnp.where(filled, SLOTS_A, counts).astype(jnp.int32)


def draw_a_cols(key, part):
    line_total = N_GY * RX * N_GZ
    base = jnp.broadcast_to(jnp.arange(KZ, dtype=jnp.int32), (line_total, KZ))
    mixed = jax.random.permutation(jax.random.fold_in(key, 21), base, axis=1, independent=True)
    return mixed[:, :SLOTS_A].reshape(N_GY, RX, N_GZ, SLOTS_A).astype(jnp.int32)


def draw_p_count(key, part):
    counts = jax.random.randint(jax.random.fold_in(key, 31), (N_GZ, KZ, N_GX), 0, SLOTS_P + 1)
    block_rows = KZ // N_GY
    picked = jax.random.randint(jax.random.fold_in(key, 32), (N_GZ, N_GY, 1, N_GX), 0, block_rows)
    position = jnp.arange(block_rows, dtype=jnp.int32)[None, None, :, None]
    filled = (position == picked).reshape(N_GZ, KZ, N_GX)
    return jnp.where(filled, SLOTS_P, counts).astype(jnp.int32)


def draw_p_cols(key, part):
    line_total = N_GZ * KZ * N_GX
    base = jnp.broadcast_to(jnp.arange(COLS_DEV, dtype=jnp.int32), (line_total, COLS_DEV))
    mixed = jax.random.permutation(jax.random.fold_in(key, 41), base, axis=1, independent=True)
    return mixed[:, :SLOTS_P].reshape(N_GZ, KZ, N_GX, SLOTS_P).astype(jnp.int32)


def shard_levels(rng, dims, cuts, least, largest):
    loudness = 1.0
    for dim, blocks in cuts:
        steps = jax.random.uniform(jax.random.fold_in(jax.random.fold_in(rng, 6), dim), (blocks,), jnp.float32, least / len(cuts), largest / len(cuts))
        loudness = loudness * jnp.repeat(jnp.exp(steps), dims[dim] // blocks).reshape((-1,) + (1,) * (len(dims) - 1 - dim))
    return loudness


def noise(own_key, shape, width, bound, cuts=(), kind=jnp.bfloat16):
    values = width * jax.random.normal(own_key, shape, jnp.float32)
    if cuts:
        values = values * shard_levels(own_key, shape, cuts, -0.22, 0.18)
    return jnp.clip(values, -bound, bound).astype(kind)


def setup_inputs(seed: int = 0) -> dict:
    key_of = jax.random.split(jax.random.key(seed), 7)
    a_vals = noise(key_of[0], (N_GY, RX, N_GZ, SLOTS_A, TILE, TILE), (4 * TILE) ** -0.5, 0.25, ((0, 4), (1, 4), (2, 2)), jnp.float32)
    a_cols = draw_a_cols(jax.random.fold_in(key_of[6], 71), 0)
    a_count = draw_a_count(jax.random.fold_in(key_of[6], 71), 0)
    p_vals = noise(key_of[3], (N_GZ, KZ, N_GX, SLOTS_P, TILE, TILE), 1.0, 6.0, ((0, 2), (1, 4), (2, 4)), jnp.float32)
    p_cols = draw_p_cols(jax.random.fold_in(key_of[6], 71), 0)
    p_count = draw_p_count(jax.random.fold_in(key_of[6], 71), 0)
    return dict(a_vals=a_vals, a_cols=a_cols, a_count=a_count, p_vals=p_vals, p_cols=p_cols, p_count=p_count)


def reference(a_vals, a_cols, a_count, p_vals, p_cols, p_count):
    tile_size = a_vals.shape[-1]
    groups_y, rows_x, slices, slots_a = a_cols.shape
    inner_rows = p_cols.shape[1]
    groups_x = p_cols.shape[2]
    slots_p = p_cols.shape[3]
    rows_all = groups_y * rows_x
    a_values = a_vals.reshape(rows_all, slices, slots_a, tile_size, tile_size)
    a_columns = a_cols.reshape(rows_all, slices, slots_a)
    a_counts = a_count.reshape(rows_all, slices)
    p_values = p_vals.reshape(slices * inner_rows, groups_x, slots_p, tile_size, tile_size)
    alive_p = jnp.arange(slots_p, dtype=jnp.int32) < p_count[..., None]
    matches = p_cols[..., None] == jnp.arange(COLS_DEV, dtype=jnp.int32)
    p_weights = (alive_p[..., None] & matches).astype(jnp.float32)
    p_weights = p_weights.reshape(slices * inner_rows, groups_x, slots_p, COLS_DEV)
    offsets = (jnp.arange(slices, dtype=jnp.int32) * inner_rows)[:, None]

    def one_row(row_index):
        alive_a = jnp.arange(slots_a, dtype=jnp.int32) < a_counts[row_index][:, None]
        tile_part = jnp.where(alive_a[..., None, None], a_values[row_index], 0.0)
        indices = a_columns[row_index].astype(jnp.int32) + offsets
        chosen = p_values[indices]
        weights = p_weights[indices]
        product = jnp.einsum("zsij,zsxpjk->zsxpik", tile_part, chosen, precision=lax.Precision.HIGHEST)
        placed = jnp.einsum("zsxpc,zsxpik->ixck", weights, product, precision=lax.Precision.HIGHEST)
        return placed.reshape(tile_size, groups_x * COLS_DEV * tile_size)

    result = lax.map(one_row, jnp.arange(rows_all, dtype=jnp.int32))
    return result.reshape(rows_all * tile_size, groups_x * COLS_DEV * tile_size)
```

```python
import functools

import jax
import jax.numpy as jnp
from jax import lax
from jax.experimental import pallas as pl
from jax.experimental.pallas import tpu as pltpu
from jax.sharding import PartitionSpec as P

COLS_DEV = 2
CUTS = 4
MESH = pl.DeviceIdType.MESH


def plan(gy):
    if gy == 4:
        opening = [(1, 0), (1, 1), (2, 1), (2, 0)]
        stages = [
            [("fwd", 0, 1, 0), ("fwd", 0, 1, 1)],
            [("fwd", 1, 1, 0), ("fwd", 1, 1, 1), ("own", 3, 0, 0), ("own", 3, 0, 1)],
            [("fwd", 2, 1, 0), ("fwd", 0, 2, 1)],
            [("fwd", 3, 1, 0), ("fwd", 1, 2, 1), ("fwd", 2, 1, 1)],
            [("fwd", 2, 2, 1), ("fwd", 3, 1, 1)],
            [("fwd", 3, 2, 1)],
        ]
        return opening, stages
    opening = [(q, rel) for q in range(1, CUTS) for rel in (0, 1)]
    waves = [[("fwd", q, d, rel) for d in range(1, gy) for rel in (0, 1)] for q in range(CUTS)]
    return opening, [[], [], waves[0], waves[1], waves[2], waves[3]]


def kernel(
    gx, gy, gz, slots_p, tiles_p,
    a_ref, p_ref, ac_ref, an_ref, pc_ref, pn_ref, o_ref,
    a_all, a_hl, p_own, p_all, ma, sa, p_mul, c_send, c_recv,
    a_recv, a_sy, a_sp, a_sf, p_load, p_recv, p_send,
    ma_recv, ma_send, s_sem, c_rs, c_ss,
):
    rows, slots, tile = a_ref.shape[0], a_ref.shape[1], a_ref.shape[2]
    blocks = p_all.shape[1]
    head = 8
    inner = tiles_p // slots_p
    rows_out = gx * rows // gz
    zero_tile = gy * inner
    width = tile // CUTS
    half = tile // 2
    part = slots // 2
    opening, stages = plan(gy)
    chips = gx // 2
    far = chips - 1
    me_x, me_y, me_z = lax.axis_index("gx"), lax.axis_index("gy"), lax.axis_index("gz")
    chip, core = me_x // 2, me_x % 2
    partner = chip * 2 + (1 - core)
    has_next = (me_y + 1 < gy, me_y >= 1)

    def remote(src, dst, send, recv, where):
        return pltpu.make_async_remote_copy(
            src_ref=src, dst_ref=dst, send_sem=send, recv_sem=recv,
            device_id=where, device_id_type=MESH)

    def arrive(ref, sem):
        pltpu.make_async_copy(ref, ref, sem).wait()

    barrier = pltpu.get_barrier_semaphore()
    for name, size, me in (("gx", gx, me_x), ("gz", gz, me_z)):
        for d in range(1, size):
            pl.semaphore_signal(
                barrier, inc=1, device_id={name: lax.rem(me + d, size)}, device_id_type=MESH
            )
    for side, step in ((0, 1), (1, -1)):
        @pl.when(has_next[side])
        def _(step=step):
            pl.semaphore_signal(
                barrier, inc=1, device_id={"gy": lax.rem(me_y + step + gy, gy)},
                device_id_type=MESH)

    load = pltpu.make_async_copy(p_ref, p_own, p_load)
    load.start()

    def a_piece(g, r, h):
        return a_all.at[g, r, pl.ds(h * part, part)]

    own_loads = []
    for r in range(rows):
        for h in (0, 1):
            own_loads.append(pltpu.make_async_copy(
                a_ref.at[r, pl.ds(h * part, part)], a_piece(me_x, r, h), a_recv.at[me_x, r, h]))
    for copy in own_loads:
        copy.start()

    line = lax.broadcasted_iota(jnp.int32, (8, 128), 0)
    lane = lax.broadcasted_iota(jnp.int32, (8, 128), 1)
    meta = jnp.zeros((8, 128), jnp.int32)
    for r in range(rows):
        for s in range(slots):
            pick = jnp.where(s < an_ref[r], ac_ref[0, r, 0, s], zero_tile)
            meta = jnp.where((line == 0) & (lane == r * slots + s), pick, meta)
    ma[me_x] = meta
    group = lax.broadcasted_iota(jnp.int32, (tile, tile), 1) // width
    group8 = lax.broadcasted_iota(jnp.int32, (8, tile), 1) // width
    for q in range(CUTS // 2):
        p_mul[q, zero_tile] = jnp.zeros_like(p_mul[q, zero_tile])

    load.wait()
    for b in range(blocks):
        mine = [b * CUTS + t for t in range(CUTS) if b * CUTS + t < tiles_p]
        code = jnp.full((8, tile), -1.0, jnp.float32)
        for n, t in enumerate(mine):
            kind = jnp.where(t % slots_p < pn_ref[t // slots_p], pc_ref[t], -1)
            code = jnp.where(group8 == n, kind.astype(jnp.float32), code)
        for q in range(CUTS):
            value = jnp.zeros((tile, tile), jnp.float32)
            for n, t in enumerate(mine):
                shift = (n - q) % CUTS * width
                turned = pltpu.roll(p_own[t], shift, 1) if shift else p_own[t]
                value = jnp.where(group == n, turned, value)
            p_all[me_y, b, head + q * tile:head + (q + 1) * tile] = value
        p_all[me_y, b, :head] = code
    for r in range(rows):
        for h in (0, 1):
            arrive(a_piece(me_x, r, h), a_recv.at[me_x, r, h])

    neighbours = jnp.where(has_next[0], 1, 0) + jnp.where(has_next[1], 1, 0)
    pl.semaphore_wait(barrier, gx + gz - 2 + neighbours)

    def p_block(src, q, b):
        if q == 0:
            return p_all.at[src, b, pl.ds(0, head + tile)]
        return p_all.at[src, b, pl.ds(head + q * tile, tile)]

    def p_copy(side, src, q, b):
        ref = p_block(src, q, b)
        step = 1 if side == 0 else -1
        return remote(ref, ref, p_send.at[side, src, q, b], p_recv.at[src, q, b],
                      {"gy": lax.rem(me_y + step + gy, gy)})

    near_side = jnp.where(2 * me_y < gy - 1, 0, 1)

    def on_side(side, rel):
        return near_side == side if rel == 0 else near_side != side

    def send_own(q, rel):
        for side in (0, 1):
            @pl.when(jnp.logical_and(on_side(side, rel), has_next[side]))
            def _(side=side):
                for b in range(blocks):
                    p_copy(side, me_y, q, b).start()

    sends = []

    def send(copy):
        copy.start()
        sends.append(copy)

    def cross(d):
        return {"gx": lax.rem(chip + d, chips) * 2 + core}

    for d in range(1, gx):
        send(remote(ma.at[me_x], ma.at[me_x], ma_send.at[d], ma_recv.at[me_x],
                    {"gx": lax.rem(me_x + d, gx)}))
    for rel in (0, 1):
        send_own(0, rel)
    for h in (0, 1):
        for d in range(1, chips):
            send(remote(a_piece(me_x, 0, h), a_piece(me_x, 0, h), a_sy.at[d, 0, h],
                        a_recv.at[me_x, 0, h], cross(d)))
    for r in list(range(1, rows)) + [0]:
        for h in (0, 1):
            send(remote(a_piece(me_x, r, h), a_piece(me_x, r, h), a_sp.at[r, h],
                        a_recv.at[me_x, r, h], {"gx": partner}))
    for q, rel in opening:
        send_own(q, rel)

    def prepare(g, r):
        values = jnp.concatenate([a_all[g, r, s] for s in range(slots)], axis=1)
        high = values.astype(jnp.bfloat16)
        a_hl[g, r, :tile] = high
        a_hl[g, r, tile:] = (values - high.astype(jnp.float32)).astype(jnp.bfloat16)

    def unpack_one(src, q):
        value = jnp.zeros((tile, tile), jnp.float32)
        for b in range(blocks):
            packed = p_all[src, b, head + q * tile:head + (q + 1) * tile]
            code = p_all[src, b, :head]
            high = packed.astype(jnp.bfloat16).astype(jnp.float32)
            low = packed - high
            turn = lambda x: [x] + [pltpu.roll(x, s * width, 1) for s in range(1, CUTS)]
            highs, lows, codes = turn(high), turn(low), turn(code)
            for n in range(CUTS):
                t = b * CUTS + n
                if t >= tiles_p:
                    continue
                parts = [highs[-n % CUTS], highs[(1 - n) % CUTS],
                         lows[(2 - n) % CUTS], lows[(3 - n) % CUTS]]
                kinds = [codes[(p - n) % CUTS] for p in range(CUTS)]
                chosen, kind = parts[3], kinds[3]
                for p in (2, 1, 0):
                    chosen = jnp.where(group == p, parts[p], chosen)
                    kind = jnp.where(group8 == p, kinds[p], kind)
                want = (group8 % COLS_DEV).astype(jnp.float32)
                keep = jnp.where(kind == want, 1.0, 0.0)
                keep = jnp.concatenate([keep] * (tile // 8), axis=0)
                placed = jnp.where(keep > 0.5, chosen, 0.0)
                value = placed if t % slots_p == 0 else value + placed
                if t % slots_p == slots_p - 1:
                    side = q % 2 * tile
                    p_mul[q // 2, src * inner + t // slots_p, :, side:side + tile] = (
                        value.astype(jnp.bfloat16))

    def source(side, d):
        src = me_y - d if side == 0 else me_y + d
        return src, src >= 0 if side == 0 else src < gy

    def forward(q, d, rel):
        for side in (0, 1):
            src, there = source(side, d)

            @pl.when(jnp.logical_and(on_side(side, rel), jnp.logical_and(there, has_next[side])))
            def _(src=src, side=side):
                for b in range(blocks):
                    arrive(p_block(src, q, b), p_recv.at[src, q, b])
                    p_copy(side, src, q, b).start()

    def advance(n):
        for kind, q, d, rel in stages[n]:
            if kind == "own":
                send_own(q, rel)
            else:
                forward(q, d, rel)

    def unpack(q):
        for d in range(1, gy):
            for side in (0, 1):
                src, there = source(side, d)

                @pl.when(there)
                def _(src=src, side=side):
                    @pl.when(jnp.logical_not(has_next[side]))
                    def _():
                        for b in range(blocks):
                            arrive(p_block(src, q, b), p_recv.at[src, q, b])
                    unpack_one(src, q)

    def chip_at(d):
        return lax.rem(chip + d, chips)

    def piece_of(g, r, h):
        return a_piece(g, r, h), a_recv.at[g, r, h]

    def relay_copies(r, o):
        copies = []
        for d in range(1, chips):
            came = lax.rem(chip - d + chips, chips)
            if r == 0:
                g, h = came * 2 + core, o
            else:
                g, h = came * 2 + o, core
            ref, sem = piece_of(g, r, h)
            copies.append((ref, sem, remote(ref, ref, a_sf.at[d, r, o], sem, {"gx": partner})))
        return copies

    def relay(r, o):
        for ref, sem, copy in relay_copies(r, o):
            arrive(ref, sem)
            copy.start()

    lanes = lax.broadcasted_iota(jnp.int32, (half, tile), 1)

    def product(g, r, cuts):
        picks = [sa[g, 0, r * slots + s] for s in range(slots)]
        first = cuts[0] % 2 * tile
        span = pl.ds(first, len(cuts) * tile)
        right = jnp.concatenate([p_mul[cuts[0] // 2, i, :, span] for i in picks], axis=0)
        out = jnp.dot(a_hl[g, r], right, preferred_element_type=jnp.float32)
        results = []
        for n in range(len(cuts)):
            both = out[:tile, n * tile:(n + 1) * tile] + out[tile:, n * tile:(n + 1) * tile]
            both = both + pltpu.roll(both, half, 1)
            results.append(jnp.where(lanes < half, both[:half], both[half:]))
        return results

    def c_copy(z, i, q):
        return remote(c_send.at[z, i, q], c_recv.at[me_z, i, q], c_ss.at[z, i, q],
                      c_rs.at[me_z, i, q], {"gz": z})

    def emit(spots, cuts):
        results = []
        for group_of in cuts:
            results += [(g, r, group_of, product(g, r, group_of)) for g, r in spots]
        for g, r, group_of, values in results:
            at = g * rows + r
            z, i = at // rows_out, lax.rem(at, rows_out)
            for q, value in zip(group_of, values):
                c_send[z, i, q] = value

            @pl.when(z != me_z)
            def _():
                for q in group_of:
                    c_copy(z, i, q).start()

    def near_row(n):
        return chip * 2 + n // rows, lax.rem(n, rows)

    def far_row(n):
        r = n // (2 * far)
        o = lax.rem(n // far, 2)
        return chip_at(1 + lax.rem(n, far)) * 2 + o, r

    n_near, n_far = 2 * rows, 2 * rows * far

    def near(q):
        emit([near_row(n) for n in range(n_near)], ((q,),))

    def far_rows(r, sides, cuts):
        for d in range(1, chips):
            emit([(chip_at(d) * 2 + o, r) for o in sides], cuts)

    def prepare_far(r, o):
        for d in range(1, chips):
            g = chip_at(d) * 2 + o
            for h in (0, 1):
                if r == 0:
                    direct = core == o
                else:
                    direct = core == h

                @pl.when(jnp.logical_not(direct))
                def _(g=g, h=h):
                    arrive(*piece_of(g, r, h))
            prepare(g, r)

    for r in range(rows):
        prepare(me_x, r)
    for r in list(range(1, rows)) + [0]:
        for h in (0, 1):
            arrive(*piece_of(partner, r, h))
    for r in range(1, rows):
        for o in (0, 1):
            for d in range(1, chips):
                ref, sem = piece_of(chip * 2 + o, r, core)
                send(remote(ref, ref, a_sy.at[d, r, o], sem, cross(d)))
    for q in range(CUTS):
        unpack_one(me_y, q)
    for d in range(1, gx):
        g = lax.rem(me_x + d, gx)
        arrive(ma.at[g], ma_recv.at[g])
    move = pltpu.make_async_copy(ma, sa, s_sem)
    move.start()
    for r in range(rows):
        prepare(partner, r)
    move.wait()

    last = n_far - far
    advance(0)
    advance(1)
    relay(0, 0)
    advance(2)
    unpack(0)
    near(0)
    advance(3)
    relay(0, 1)
    unpack(1)
    near(1)
    prepare_far(0, 0)
    prepare_far(0, 1)
    advance(4)
    far_rows(0, (0, 1), ((0, 1),))
    advance(5)
    for r in range(1, rows):
        for o in (0, 1):
            if (r, o) != (rows - 1, 1):
                relay(r, o)
                prepare_far(r, o)
                far_rows(r, (o,), ((0, 1),))
    unpack(2)
    near(2)
    far_rows(0, (0, 1), ((2,),))
    for r in range(1, rows):
        for o in (0, 1):
            if (r, o) != (rows - 1, 1):
                far_rows(r, (o,), ((2,),))
    unpack(3)
    near_mine = (chip * n_near) // rows_out == me_z
    total = n_near + (last if rows > 1 else n_far)
    begin = jnp.where(near_mine, n_near, 0)

    def mixed(n):
        m = lax.rem(n + begin, total)
        is_near = m < n_near
        g0, r0 = near_row(m)
        g1, r1 = far_row(jnp.maximum(m - n_near, 0)) if far else (g0, r0)
        return jnp.where(is_near, g0, g1), jnp.where(is_near, r0, r1)

    early = min(3, total)
    emit([mixed(n) for n in range(early)], ((3,),))
    if rows > 1:
        relay(rows - 1, 1)
    emit([mixed(n) for n in range(early, total)], ((3,),))
    if rows > 1:
        prepare_far(rows - 1, 1)
        far_rows(rows - 1, (1,), ((0, 1), (2, 3)))

    def finish(i):
        top = [None, None]
        low = [None, None]
        spot = lanes // width
        for q in range(CUTS):
            value = c_send[me_z, i, q]
            for d in range(1, gz):
                z = lax.rem(me_z + d, gz)
                arrive(c_recv.at[z, i, q], c_rs.at[z, i, q])
                value = value + c_recv[z, i, q]
            turned = [value] + [pltpu.roll(value, s * width, 1) for s in range(1, CUTS)]
            for c in range(COLS_DEV):
                for store, base in ((top, c), (low, c + COLS_DEV)):
                    piece = turned[(q - base) % CUTS]
                    store[c] = piece if q == 0 else jnp.where(spot == q, piece, store[c])
        for c in range(COLS_DEV):
            o_ref[pl.ds(i * tile, half), c * tile:(c + 1) * tile] = top[c]
            o_ref[pl.ds(i * tile + half, half), c * tile:(c + 1) * tile] = low[c]

    for r in range(rows):
        for i in range(r, rows_out, rows):
            finish(i)

    for copy in sends:
        copy.wait_send()
    for r in range(rows):
        for o in (0, 1):
            for _, _, copy in relay_copies(r, o):
                copy.wait_send()
    for side in (0, 1):
        for d in range(0, gy):
            src, there = source(side, d)

            @pl.when(jnp.logical_and(there, has_next[side]))
            def _(src=src, side=side):
                for q in range(CUTS):
                    for b in range(blocks):
                        p_copy(side, src, q, b).wait_send()
    for d in range(1, gz):
        z = lax.rem(me_z + d, gz)
        for i in range(rows_out):
            for q in range(CUTS):
                c_copy(z, i, q).wait_send()


def body(gx, gy, gz, a_vals, a_cols, a_count, p_vals, p_cols, p_count):
    if a_vals.shape[3] % 2:
        wide = [(0, 0)] * 3 + [(0, 1)]
        a_vals = jnp.pad(a_vals, wide + [(0, 0)] * 2)
        a_cols = jnp.pad(a_cols, wide)
    rows, slots, tile = a_vals.shape[1], a_vals.shape[3], a_vals.shape[-1]
    inner, slots_p = p_vals.shape[1], p_vals.shape[3]
    tiles_p = inner * slots_p
    blocks = -(-tiles_p // CUTS)
    rows_out = gx * rows // gz
    chips = max(gx // 2, 1)
    dma = pltpu.SemaphoreType.DMA
    any_spec = pl.BlockSpec(memory_space=pl.ANY)
    smem_spec = pl.BlockSpec(memory_space=pltpu.SMEM)
    return pl.pallas_call(
        functools.partial(kernel, gx, gy, gz, slots_p, tiles_p),
        out_shape=pltpu.VMEM((rows_out * tile, COLS_DEV * tile), jnp.float32),
        in_specs=[any_spec] * 2 + [smem_spec] * 4,
        out_specs=pl.BlockSpec(memory_space=pltpu.VMEM),
        scratch_shapes=[
            pltpu.VMEM((gx, rows, slots, tile, tile), jnp.float32),
            pltpu.VMEM((gx, rows, 2 * tile, slots * tile), jnp.bfloat16),
            pltpu.VMEM((tiles_p, tile, tile), jnp.float32),
            pltpu.VMEM((gy, blocks, 8 + CUTS * tile, tile), jnp.float32),
            pltpu.VMEM((gx, 8, 128), jnp.int32),
            pltpu.SMEM((gx, 8, 128), jnp.int32),
            pltpu.VMEM((CUTS // 2, gy * inner + 1, tile, 2 * tile), jnp.bfloat16),
            pltpu.VMEM((gz, rows_out, CUTS, tile // 2, tile), jnp.float32),
            pltpu.VMEM((gz, rows_out, CUTS, tile // 2, tile), jnp.float32),
            dma((gx, rows, 2)),
            dma((chips, rows, 2)),
            dma((rows, 2)),
            dma((chips, rows, 2)),
            dma,
            dma((gy, CUTS, blocks)),
            dma((2, gy, CUTS, blocks)),
            dma((gx,)),
            dma((gx,)),
            dma,
            dma((gz, rows_out, CUTS)),
            dma((gz, rows_out, CUTS)),
        ],
        compiler_params=pltpu.CompilerParams(collective_id=0, has_side_effects=True),
    )(
        a_vals[0, :, 0], p_vals.reshape(tiles_p, tile, tile),
        a_cols, a_count.reshape(-1), p_cols.reshape(-1), p_count.reshape(-1),
    )


def solution(mesh):
    placed = (
        P("gy", "gx", "gz", None, None, None),
        P("gy", "gx", "gz", None),
        P("gy", "gx", "gz"),
        P("gz", "gy", "gx", None, None, None),
        P("gz", "gy", "gx", None),
        P("gz", "gy", "gx"),
    )
    sizes = (mesh.shape["gx"], mesh.shape["gy"], mesh.shape["gz"])
    return jax.shard_map(
        functools.partial(body, *sizes),
        mesh=mesh, in_specs=placed, out_specs=P(("gy", "gz"), "gx"), check_vma=False,
    )
```

```python
import functools

import jax
import jax.numpy as jnp
from jax import lax
from jax.experimental import pallas as pl
from jax.experimental.pallas import tpu as pltpu
from jax.sharding import PartitionSpec as P

COLS_DEV = 2
CUTS = 4
MESH = pl.DeviceIdType.MESH


def plan(gy):
    if gy == 4:
        opening = [(1, 0), (1, 1), (2, 1), (2, 0)]
        stages = [
            [("fwd", 0, 1, 1), ("fwd", 0, 1, 0)],
            [("fwd", 1, 1, 1), ("fwd", 1, 1, 0)],
            [("fwd", 2, 1, 0), ("fwd", 2, 1, 1), ("mid", 3, 0, 0), ("mid", 3, 0, 1)],
            [("fwd", 3, 1, 0)],
            [("fwd", 2, 2, 1), ("fwd", 3, 1, 1)],
            [("fwd", 3, 2, 1)],
        ]
        return opening, stages, 2
    opening = [(q, rel) for q in range(1, CUTS) for rel in (0, 1)]
    waves = [[("fwd", q, d, rel) for d in range(1, gy) for rel in (0, 1)] for q in range(CUTS)]
    return opening, [[], [], waves[0], waves[1], waves[2], waves[3]], 0


def kernel(
    gx, gy, gz, slots_p, tiles_p,
    a_ref, p_ref, ac_ref, an_ref, pc_ref, pn_ref, o_ref,
    a_all, a_hl, p_own, p_all, ma, sa, p_mul, c_send, c_recv,
    a_recv, a_sy, a_sp, a_sf, p_load, p_recv, p_send,
    ma_recv, ma_send, s_sem, c_rs, c_ss, far_ok, far_send,
):
    rows, slots, tile = a_ref.shape[0], a_ref.shape[1], a_ref.shape[2]
    blocks = p_all.shape[1]
    head = 8
    inner = tiles_p // slots_p
    rows_out = gx * rows // gz
    zero_tile = gy * inner
    width = tile // CUTS
    half = tile // 2
    quarter = half // 2
    part = slots // 2
    opening, stages, straight = plan(gy)
    chips = gx // 2
    far = chips - 1
    me_x, me_y, me_z = lax.axis_index("gx"), lax.axis_index("gy"), lax.axis_index("gz")
    chip, core = me_x // 2, me_x % 2
    partner = chip * 2 + (1 - core)
    has_next = (me_y + 1 < gy, me_y >= 1)

    def remote(src, dst, send, recv, where):
        return pltpu.make_async_remote_copy(
            src_ref=src, dst_ref=dst, send_sem=send, recv_sem=recv,
            device_id=where, device_id_type=MESH)

    def arrive(ref, sem):
        pltpu.make_async_copy(ref, ref, sem).wait()

    barrier = pltpu.get_barrier_semaphore()
    for name, size, me in (("gx", gx, me_x), ("gz", gz, me_z)):
        for d in range(1, size):
            pl.semaphore_signal(
                barrier, inc=1, device_id={name: lax.rem(me + d, size)}, device_id_type=MESH
            )
    for side, step in ((0, 1), (1, -1)):
        @pl.when(has_next[side])
        def _(step=step):
            pl.semaphore_signal(
                barrier, inc=1, device_id={"gy": lax.rem(me_y + step + gy, gy)},
                device_id_type=MESH)

    load = pltpu.make_async_copy(p_ref, p_own, p_load)
    load.start()

    def a_piece(g, r, h, v):
        at = pl.ds(v * half, half)
        if r == 0:
            return a_all.at[g, 0, :, at], a_recv.at[g, v]
        return (a_all.at[g, r, pl.ds(h * part, part), at],
                a_recv.at[g, 2 + (r - 1) * 4 + h * 2 + v])

    own_loads = [pltpu.make_async_copy(a_ref.at[r], a_all.at[me_x, r], a_recv.at[me_x, r])
                 for r in range(rows)]
    for copy in own_loads:
        copy.start()

    line = lax.broadcasted_iota(jnp.int32, (8, 128), 0)
    lane = lax.broadcasted_iota(jnp.int32, (8, 128), 1)
    meta = jnp.zeros((8, 128), jnp.int32)
    for r in range(rows):
        for s in range(slots):
            pick = jnp.where(s < an_ref[r], ac_ref[0, r, 0, s], zero_tile)
            meta = jnp.where((line == 0) & (lane == r * slots + s), pick, meta)
    ma[me_x] = meta
    group = lax.broadcasted_iota(jnp.int32, (tile, tile), 1) // width
    group8 = lax.broadcasted_iota(jnp.int32, (8, tile), 1) // width
    for q in range(CUTS // 2):
        p_mul[q, zero_tile] = jnp.zeros_like(p_mul[q, zero_tile])

    load.wait()
    for b in range(blocks):
        mine = [b * CUTS + t for t in range(CUTS) if b * CUTS + t < tiles_p]
        code = jnp.full((8, tile), -1.0, jnp.float32)
        for n, t in enumerate(mine):
            kind = jnp.where(t % slots_p < pn_ref[t // slots_p], pc_ref[t], -1)
            code = jnp.where(group8 == n, kind.astype(jnp.float32), code)
        for q in range(CUTS):
            value = jnp.zeros((tile, tile), jnp.float32)
            for n, t in enumerate(mine):
                shift = (n - q) % CUTS * width
                turned = pltpu.roll(p_own[t], shift, 1) if shift else p_own[t]
                value = jnp.where(group == n, turned, value)
            p_all[me_y, b, head + q * tile:head + (q + 1) * tile] = value
        p_all[me_y, b, :head] = code
    for r in range(rows):
        arrive(a_all.at[me_x, r], a_recv.at[me_x, r])

    neighbours = jnp.where(has_next[0], 1, 0) + jnp.where(has_next[1], 1, 0)
    pl.semaphore_wait(barrier, gx + gz - 2 + neighbours)

    def p_block(src, q, b):
        if q == 0:
            return p_all.at[src, b, pl.ds(0, head + tile)]
        return p_all.at[src, b, pl.ds(head + q * tile, tile)]

    def p_copy(side, src, q, b):
        ref = p_block(src, q, b)
        step = 1 if side == 0 else -1
        return remote(ref, ref, p_send.at[side, src], p_recv.at[src, q, b],
                      {"gy": lax.rem(me_y + step + gy, gy)})

    near_side = jnp.where(2 * me_y < gy - 1, 0, 1)

    def on_side(side, rel):
        return near_side == side if rel == 0 else near_side != side

    def send_own(q, rel, only=True):
        for side in (0, 1):
            @pl.when(jnp.logical_and(only, jnp.logical_and(on_side(side, rel), has_next[side])))
            def _(side=side):
                for b in range(blocks):
                    p_copy(side, me_y, q, b).start()

    between = jnp.logical_and(has_next[0], has_next[1])
    onward = jnp.where(near_side == 0, 1, -1)

    def tell(step):
        pl.semaphore_signal(far_ok, inc=1, device_id={"gy": me_y + step}, device_id_type=MESH)

    if straight:
        @pl.when(between)
        def _():
            tell(onward)

    def send(copy):
        copy.start()

    def cross(d):
        return {"gx": lax.rem(chip + d, chips) * 2 + core}

    for d in range(1, gx):
        send(remote(ma.at[me_x], ma.at[me_x], ma_send, ma_recv,
                    {"gx": lax.rem(me_x + d, gx)}))
    for rel in (0, 1):
        send_own(0, rel)
    for v in (0, 1):
        for d in range(1, chips):
            ref, sem = a_piece(me_x, 0, 0, v)
            send(remote(ref, ref, a_sy.at[d], sem, cross(d)))
    for r in list(range(1, rows)) + [0]:
        send(remote(a_all.at[me_x, r], a_all.at[me_x, r], a_sp,
                    a_recv.at[me_x, r], {"gx": partner}))
    for q, rel in opening:
        send_own(q, rel)

    def prepare(g, r, v):
        at = pl.ds(v * half, half)
        values = jnp.concatenate([a_all[g, r, s, at] for s in range(slots)], axis=1)
        high = values.astype(jnp.bfloat16)
        a_hl[g, r, v * half:(v + 1) * half] = high
        low = (values - high.astype(jnp.float32)).astype(jnp.bfloat16)
        a_hl[g, r, tile + v * half:tile + (v + 1) * half] = low

    def unpack_one(src, q):
        value = jnp.zeros((tile, tile), jnp.float32)
        for b in range(blocks):
            packed = p_all[src, b, head + q * tile:head + (q + 1) * tile]
            code = p_all[src, b, :head]
            high = packed.astype(jnp.bfloat16).astype(jnp.float32)
            low = packed - high
            turn = lambda x: [x] + [pltpu.roll(x, s * width, 1) for s in range(1, CUTS)]
            highs, lows, codes = turn(high), turn(low), turn(code)
            for n in range(CUTS):
                t = b * CUTS + n
                if t >= tiles_p:
                    continue
                parts = [highs[-n % CUTS], highs[(1 - n) % CUTS],
                         lows[(2 - n) % CUTS], lows[(3 - n) % CUTS]]
                kinds = [codes[(p - n) % CUTS] for p in range(CUTS)]
                chosen, kind = parts[3], kinds[3]
                for p in (2, 1, 0):
                    chosen = jnp.where(group == p, parts[p], chosen)
                    kind = jnp.where(group8 == p, kinds[p], kind)
                want = (group8 % COLS_DEV).astype(jnp.float32)
                keep = jnp.where(kind == want, 1.0, 0.0)
                keep = jnp.concatenate([keep] * (tile // 8), axis=0)
                placed = jnp.where(keep > 0.5, chosen, 0.0)
                value = placed if t % slots_p == 0 else value + placed
                if t % slots_p == slots_p - 1:
                    side = q % 2 * tile
                    p_mul[q // 2, src * inner + t // slots_p, :, side:side + tile] = (
                        value.astype(jnp.bfloat16))

    def source(side, d):
        src = me_y - d if side == 0 else me_y + d
        return src, src >= 0 if side == 0 else src < gy

    def forward(q, d, rel):
        for side in (0, 1):
            src, there = source(side, d)

            @pl.when(jnp.logical_and(on_side(side, rel), jnp.logical_and(there, has_next[side])))
            def _(src=src, side=side):
                for b in range(blocks):
                    arrive(p_block(src, q, b), p_recv.at[src, q, b])
                    p_copy(side, src, q, b).start()

    def advance(n):
        for kind, q, d, rel in stages[n]:
            if kind == "own":
                send_own(q, rel)
            elif kind == "mid":
                send_own(q, rel, between)
            else:
                forward(q, d, rel)

    def unpack(q):
        for d in range(1, gy):
            for side in (0, 1):
                src, there = source(side, d)

                @pl.when(there)
                def _(src=src, side=side):
                    loose = q < straight and d == 2

                    @pl.when(True if loose else jnp.logical_not(has_next[side]))
                    def _():
                        for b in range(blocks):
                            arrive(p_block(src, q, b), p_recv.at[src, q, b])
                    unpack_one(src, q)

    def chip_at(d):
        return lax.rem(chip + d, chips)

    def relay_copies(r, o, v):
        copies = []
        for d in range(1, chips):
            came = lax.rem(chip - d + chips, chips)
            g = came * 2 + (core if r == 0 else o)
            ref, sem = a_piece(g, r, core, v)
            copies.append((ref, sem, remote(
                ref, ref, a_sf.at[d], sem, {"gx": partner})))
        return copies

    def relay(r, o, v):
        for ref, sem, copy in relay_copies(r, o, v):
            arrive(ref, sem)
            copy.start()

    lane_id = lax.broadcasted_iota(jnp.int32, (quarter, tile), 1)

    def product(g, r, v, cuts):
        picks = [sa[g, 0, r * slots + s] for s in range(slots)]
        first = cuts[0] % 2 * tile
        span = pl.ds(first, len(cuts) * tile)
        right = jnp.concatenate([p_mul[cuts[0] // 2, i, :, span] for i in picks], axis=0)
        if v is None:
            left, size = a_hl[g, r], tile
        else:
            left, size = jnp.concatenate(
                [a_hl[g, r, pl.ds(b + v * half, half)] for b in (0, tile)], axis=0), half
        out = jnp.dot(left, right, preferred_element_type=jnp.float32)
        results = []
        for n in range(len(cuts)):
            both = out[:size, n * tile:(n + 1) * tile] + out[size:, n * tile:(n + 1) * tile]
            both = both + pltpu.roll(both, half, 1)
            results.append(jnp.concatenate(
                [jnp.where(lane_id < half, both[b:b + quarter], both[b + quarter:b + half])
                 for b in range(0, size, half)], axis=0))
        return results

    def c_copy(z, i, q, v=None):
        at = pl.ds(0, half) if v is None else pl.ds(v * quarter, quarter)
        return remote(c_send.at[z, i, q, at], c_recv.at[me_z, i, q, at], c_ss.at[z],
                      c_rs.at[lax.rem(me_z - z - 1 + 2 * gz, gz), i, q // (CUTS - 1)], {"gz": z})

    def emit(spots, cuts):
        results = []
        for group_of in cuts:
            results += [(g, r, v, group_of, product(g, r, v, group_of)) for g, r, v in spots]
        for g, r, v, group_of, values in results:
            at = g * rows + r
            z, i = at // rows_out, lax.rem(at, rows_out)
            for q, value in zip(group_of, values):
                if v is None:
                    c_send[z, i, q] = value
                else:
                    c_send[z, i, q, v * quarter:(v + 1) * quarter] = value

            @pl.when(z != me_z)
            def _():
                for q in group_of:
                    c_copy(z, i, q, v).start()

    def near_row(n):
        return chip * 2 + n // rows, lax.rem(n, rows)

    def far_row(n):
        r = n // (2 * far)
        o = lax.rem(n // far, 2)
        return chip_at(1 + lax.rem(n, far)) * 2 + o, r

    n_near, n_far = 2 * rows, 2 * rows * far

    def near(q):
        emit([near_row(n) + (None,) for n in range(n_near)], ((q,),))

    def far_rows(r, sides, v, cuts):
        for d in range(1, chips):
            emit([(chip_at(d) * 2 + o, r, v) for o in sides], cuts)

    def prepare_far(r, sides, v):
        for d in range(1, chips):
            for o in sides:
                g = chip_at(d) * 2 + o
                for h in (0,) if r == 0 else (0, 1):
                    direct = core == (o if r == 0 else h)

                    @pl.when(jnp.logical_not(direct))
                    def _(g=g, h=h):
                        arrive(*a_piece(g, r, h, v))
                prepare(g, r, v)

    for r in range(rows):
        for v in (0, 1):
            prepare(me_x, r, v)
    if straight:
        @pl.when(between)
        def _():
            pl.semaphore_wait(far_ok, 1)
            tell(-onward)
    for r in list(range(1, rows)) + [0]:
        arrive(a_all.at[partner, r], a_recv.at[partner, r])
    for r in range(1, rows):
        for o in (0, 1):
            for v in (0, 1):
                for d in range(1, chips):
                    ref, sem = a_piece(chip * 2 + o, r, core, v)
                    send(remote(ref, ref, a_sy.at[d], sem, cross(d)))
    if straight:
        @pl.when(jnp.logical_not(between))
        def _():
            pl.semaphore_wait(far_ok, 1)
            for q in range(straight):
                for b in range(blocks):
                    ref = p_block(me_y, q, b)
                    remote(ref, ref, far_send, p_recv.at[me_y, q, b],
                           {"gy": gy - 1 - me_y}).start()
            send_own(CUTS - 1, 0)
    for q in range(CUTS):
        unpack_one(me_y, q)
    arrive(ma.at[pl.ds(0, gx - 1)], ma_recv)
    move = pltpu.make_async_copy(ma, sa, s_sem)
    move.start()
    for r in range(rows):
        for v in (0, 1):
            prepare(partner, r, v)
    move.wait()

    last_row = (rows - 1, 1)
    middle = [(r, o) for r in range(1, rows) for o in (0, 1) if (r, o) != last_row]
    both = (0, 1)
    near_mine = (chip * n_near) // rows_out == me_z

    def all_rows(n_more):
        total = n_near + n_more
        begin = jnp.where(near_mine, n_near, 0)
        spots = []
        for n in range(total):
            m = lax.rem(n + begin, total)
            is_near = m < n_near
            g0, r0 = near_row(m)
            g1, r1 = far_row(jnp.maximum(m - n_near, 0)) if far else (g0, r0)
            spots.append((jnp.where(is_near, g0, g1), jnp.where(is_near, r0, r1), None))
        return spots

    def sweep(spots, q):
        for n in range(0, len(spots), 3):
            emit(spots[n:n + 3], ((q,),))

    n_first = 2 * far
    advance(0)
    advance(1)
    relay(0, 0, 0)
    advance(2)
    advance(3)
    prepare_far(0, both, 0)
    unpack(0)
    relay(0, 0, 1)
    far_rows(0, both, 0, ((0,),))
    near(0)
    unpack(1)
    far_rows(0, both, 0, ((1,),))
    near(1)
    advance(4)
    prepare_far(0, both, 1)
    far_rows(0, both, 1, ((0, 1),))
    for v in both:
        for r, o in middle:
            relay(r, o, v)
    advance(5)
    for v in both:
        for r, o in middle:
            prepare_far(r, (o,), v)
            far_rows(r, (o,), v, ((0, 1),))
    unpack(2)
    if rows > 1:
        relay(*last_row, 0)
    sweep(all_rows(n_far - far if rows > 1 else n_far), 2)
    unpack(3)
    spots = all_rows(n_far - far if rows > 1 else n_far)
    sweep(spots[:3], 3)
    if rows > 1:
        prepare_far(rows - 1, (1,), 0)
        relay(*last_row, 1)
        far_rows(rows - 1, (1,), 0, ((0, 1), (2, 3)))
    emit(spots[3:], ((3,),))
    if rows > 1:
        prepare_far(rows - 1, (1,), 1)
        far_rows(rows - 1, (1,), 1, ((0, 1), (2, 3)))

    lanes = lax.broadcasted_iota(jnp.int32, (half, tile), 1)

    spot = lanes // width

    def finish(n, cuts, fresh):
        i = jnp.where(near_mine, n, n % (rows_out // rows) * rows + n // (rows_out // rows))
        top = [None, None]
        low = [None, None]
        for d in range(1, gz):
            z = lax.rem(me_z + d, gz)
            arrive(c_recv.at[z, i, pl.ds(cuts[0], len(cuts))], c_rs.at[d - 1, i, 0 if fresh else 1])
        for q in cuts:
            value = c_send[me_z, i, q]
            for d in range(1, gz):
                value = value + c_recv[lax.rem(me_z + d, gz), i, q]
            turned = [value] + [pltpu.roll(value, s * width, 1) for s in range(1, CUTS)]
            for c in range(COLS_DEV):
                for store, base in ((top, c), (low, c + COLS_DEV)):
                    piece = turned[(q - base) % CUTS]
                    old = store[c]
                    store[c] = piece if old is None else jnp.where(spot == q, piece, old)
        ours = spot >= cuts[0]
        for c in range(COLS_DEV):
            lane_to = slice(c * tile, (c + 1) * tile)
            for b in (0, 1):
                for e, store in enumerate((top, low)):
                    to = pl.ds(pl.multiple_of(i * tile + b * half + e * quarter, quarter), quarter)
                    at = slice(b * quarter, (b + 1) * quarter)
                    value = store[c][at]
                    if not fresh:
                        value = jnp.where(ours[at], value, o_ref[to, lane_to])
                    o_ref[to, lane_to] = value

    for n in range(rows_out):
        finish(n, range(CUTS - 1), True)
    for n in range(rows_out):
        finish(n, (CUTS - 1,), False)

    arrive(ma.at[pl.ds(0, gx - 1)], ma_send)
    for d in range(1, chips):
        arrive(a_all.at[me_x], a_sy.at[d])
        arrive(a_all.at[me_x], a_sf.at[d])
    arrive(a_all.at[me_x], a_sp)
    for side in (0, 1):
        for d in range(0, gy):
            src, there = source(side, d)

            @pl.when(jnp.logical_and(there, has_next[side]))
            def _(src=src, side=side, d=d):
                skip = head + straight * tile if straight and d == 2 else 0
                ref = p_all.at[src, :, pl.ds(skip, head + CUTS * tile - skip)]
                arrive(ref, p_send.at[side, src])
    if straight:
        @pl.when(jnp.logical_not(between))
        def _():
            arrive(p_all.at[me_y, :, pl.ds(0, head + straight * tile)], far_send)
    for d in range(1, gz):
        z = lax.rem(me_z + d, gz)
        arrive(c_send.at[z], c_ss.at[z])


def body(gx, gy, gz, a_vals, a_cols, a_count, p_vals, p_cols, p_count):
    if a_vals.shape[3] % 2:
        wide = [(0, 0)] * 3 + [(0, 1)]
        a_vals = jnp.pad(a_vals, wide + [(0, 0)] * 2)
        a_cols = jnp.pad(a_cols, wide)
    rows, slots, tile = a_vals.shape[1], a_vals.shape[3], a_vals.shape[-1]
    inner, slots_p = p_vals.shape[1], p_vals.shape[3]
    tiles_p = inner * slots_p
    blocks = -(-tiles_p // CUTS)
    rows_out = gx * rows // gz
    chips = max(gx // 2, 1)
    dma = pltpu.SemaphoreType.DMA
    any_spec = pl.BlockSpec(memory_space=pl.ANY)
    smem_spec = pl.BlockSpec(memory_space=pltpu.SMEM)
    return pl.pallas_call(
        functools.partial(kernel, gx, gy, gz, slots_p, tiles_p),
        out_shape=pltpu.VMEM((rows_out * tile, COLS_DEV * tile), jnp.float32),
        in_specs=[any_spec] * 2 + [smem_spec] * 4,
        out_specs=pl.BlockSpec(memory_space=pltpu.VMEM),
        scratch_shapes=[
            pltpu.VMEM((gx, rows, slots, tile, tile), jnp.float32),
            pltpu.VMEM((gx, rows, 2 * tile, slots * tile), jnp.bfloat16),
            pltpu.VMEM((tiles_p, tile, tile), jnp.float32),
            pltpu.VMEM((gy, blocks, 8 + CUTS * tile, tile), jnp.float32),
            pltpu.VMEM((gx, 8, 128), jnp.int32),
            pltpu.SMEM((gx, 8, 128), jnp.int32),
            pltpu.VMEM((CUTS // 2, gy * inner + 1, tile, 2 * tile), jnp.bfloat16),
            pltpu.VMEM((gz, rows_out, CUTS, tile // 2, tile), jnp.float32),
            pltpu.VMEM((gz, rows_out, CUTS, tile // 2, tile), jnp.float32),
            dma((gx, max(4 * rows - 2, rows))),
            dma((chips,)),
            dma,
            dma((chips,)),
            dma,
            dma((gy, CUTS, blocks)),
            dma((2, gy)),
            dma,
            dma,
            dma,
            dma((max(gz - 1, 1), rows_out, 2)),
            dma((gz,)),
            pltpu.SemaphoreType.REGULAR,
            dma,
        ],
        compiler_params=pltpu.CompilerParams(collective_id=0, has_side_effects=True),
    )(
        a_vals[0, :, 0], p_vals.reshape(tiles_p, tile, tile),
        a_cols, a_count.reshape(-1), p_cols.reshape(-1), p_count.reshape(-1),
    )


def solution(mesh):
    placed = (
        P("gy", "gx", "gz", None, None, None),
        P("gy", "gx", "gz", None),
        P("gy", "gx", "gz"),
        P("gz", "gy", "gx", None, None, None),
        P("gz", "gy", "gx", None),
        P("gz", "gy", "gx"),
    )
    sizes = (mesh.shape["gx"], mesh.shape["gy"], mesh.shape["gz"])
    return jax.shard_map(
        functools.partial(body, *sizes),
        mesh=mesh, in_specs=placed, out_specs=P(("gy", "gz"), "gx"), check_vma=False,
    )
```

```python
import functools

import jax
import jax.numpy as jnp
from jax import lax
from jax.experimental import pallas as pl
from jax.experimental.pallas import tpu as pltpu
from jax.sharding import PartitionSpec as P

COLS_DEV = 2
CUTS = 4
MESH = pl.DeviceIdType.MESH


def plan(gy):
    if gy == 4:
        opening = [(1, 0), (1, 1), (2, 1), (2, 0)]
        stages = [
            [("fwd", 0, 1, 1), ("fwd", 0, 1, 0)],
            [("fwd", 1, 1, 1), ("fwd", 1, 1, 0)],
            [("fwd", 2, 1, 0), ("fwd", 2, 1, 1), ("mid", 3, 0, 0), ("mid", 3, 0, 1)],
            [("fwd", 3, 1, 0)],
            [("fwd", 2, 2, 1)],
            [("fwd", 3, 1, 1)],
            [("fwd", 3, 2, 1)],
        ]
        return opening, stages, 2
    opening = [(q, rel) for q in range(1, CUTS) for rel in (0, 1)]
    waves = [[("fwd", q, d, rel) for d in range(1, gy) for rel in (0, 1)] for q in range(CUTS)]
    return opening, [[], [], waves[0], waves[1], waves[2], [], waves[3]], 0


def kernel(
    gx, gy, gz, slots_p, tiles_p,
    a_ref, p_ref, ac_ref, an_ref, pc_ref, pn_ref, o_ref,
    a_all, a_hl, p_own, p_all, ma, sa, p_mul, c_send, c_recv,
    a_recv, a_sy, a_sp, a_sf, p_load, p_recv, p_send,
    ma_recv, ma_send, s_sem, c_rs, c_ss, far_ok, far_send,
):
    rows, slots, tile = a_ref.shape[0], a_ref.shape[1], a_ref.shape[2]
    blocks = p_all.shape[1]
    head = 8
    inner = tiles_p // slots_p
    rows_out = gx * rows // gz
    zero_tile = gy * inner
    width = tile // CUTS
    half = tile // 2
    quarter = half // 2
    part = slots // 2
    opening, stages, straight = plan(gy)
    chips = gx // 2
    far = chips - 1
    me_x, me_y, me_z = lax.axis_index("gx"), lax.axis_index("gy"), lax.axis_index("gz")
    chip, core = me_x // 2, me_x % 2
    partner = chip * 2 + (1 - core)
    has_next = (me_y + 1 < gy, me_y >= 1)

    def remote(src, dst, send, recv, where):
        return pltpu.make_async_remote_copy(
            src_ref=src, dst_ref=dst, send_sem=send, recv_sem=recv,
            device_id=where, device_id_type=MESH)

    def arrive(ref, sem):
        pltpu.make_async_copy(ref, ref, sem).wait()

    barrier = pltpu.get_barrier_semaphore()
    for name, size, me in (("gx", gx, me_x), ("gz", gz, me_z)):
        for d in range(1, size):
            pl.semaphore_signal(
                barrier, inc=1, device_id={name: lax.rem(me + d, size)}, device_id_type=MESH
            )
    for side, step in ((0, 1), (1, -1)):
        @pl.when(has_next[side])
        def _(step=step):
            pl.semaphore_signal(
                barrier, inc=1, device_id={"gy": lax.rem(me_y + step + gy, gy)},
                device_id_type=MESH)

    load = pltpu.make_async_copy(p_ref, p_own, p_load)
    load.start()

    def a_piece(g, r, h, v):
        at = pl.ds(v * half, half)
        if r == 0:
            return a_all.at[g, 0, :, at], a_recv.at[g, v]
        return (a_all.at[g, r, pl.ds(h * part, part), at],
                a_recv.at[g, 2 + (r - 1) * 4 + h * 2 + v])

    own_loads = [pltpu.make_async_copy(a_ref.at[r], a_all.at[me_x, r], a_recv.at[me_x, r])
                 for r in range(rows)]
    for copy in own_loads:
        copy.start()

    line = lax.broadcasted_iota(jnp.int32, (8, 128), 0)
    lane = lax.broadcasted_iota(jnp.int32, (8, 128), 1)
    meta = jnp.zeros((8, 128), jnp.int32)
    for r in range(rows):
        for s in range(slots):
            pick = jnp.where(s < an_ref[r], ac_ref[0, r, 0, s], zero_tile)
            meta = jnp.where((line == 0) & (lane == r * slots + s), pick, meta)
    ma[me_x] = meta
    group = lax.broadcasted_iota(jnp.int32, (tile, tile), 1) // width
    group8 = lax.broadcasted_iota(jnp.int32, (8, tile), 1) // width
    for q in range(CUTS // 2):
        p_mul[q, zero_tile] = jnp.zeros_like(p_mul[q, zero_tile])

    load.wait()
    for b in range(blocks):
        mine = [b * CUTS + t for t in range(CUTS) if b * CUTS + t < tiles_p]
        code = jnp.full((8, tile), -1.0, jnp.float32)
        for n, t in enumerate(mine):
            kind = jnp.where(t % slots_p < pn_ref[t // slots_p], pc_ref[t], -1)
            code = jnp.where(group8 == n, kind.astype(jnp.float32), code)
        for q in range(CUTS):
            value = jnp.zeros((tile, tile), jnp.float32)
            for n, t in enumerate(mine):
                shift = (n - q) % CUTS * width
                turned = pltpu.roll(p_own[t], shift, 1) if shift else p_own[t]
                value = jnp.where(group == n, turned, value)
            p_all[me_y, b, head + q * tile:head + (q + 1) * tile] = value
        p_all[me_y, b, :head] = code
    for r in range(rows):
        arrive(a_all.at[me_x, r], a_recv.at[me_x, r])

    neighbours = jnp.where(has_next[0], 1, 0) + jnp.where(has_next[1], 1, 0)
    pl.semaphore_wait(barrier, gx + gz - 2 + neighbours)

    def p_block(src, q, b):
        if q == 0:
            return p_all.at[src, b, pl.ds(0, head + tile)]
        return p_all.at[src, b, pl.ds(head + q * tile, tile)]

    def p_copy(side, src, q, b):
        ref = p_block(src, q, b)
        step = 1 if side == 0 else -1
        return remote(ref, ref, p_send.at[side, src], p_recv.at[src, q, b],
                      {"gy": lax.rem(me_y + step + gy, gy)})

    near_side = jnp.where(2 * me_y < gy - 1, 0, 1)

    def on_side(side, rel):
        return near_side == side if rel == 0 else near_side != side

    def send_own(q, rel, only=True):
        for side in (0, 1):
            @pl.when(jnp.logical_and(only, jnp.logical_and(on_side(side, rel), has_next[side])))
            def _(side=side):
                for b in range(blocks):
                    p_copy(side, me_y, q, b).start()

    between = jnp.logical_and(has_next[0], has_next[1])
    onward = jnp.where(near_side == 0, 1, -1)

    def tell(step):
        pl.semaphore_signal(far_ok, inc=1, device_id={"gy": me_y + step}, device_id_type=MESH)

    if straight:
        @pl.when(between)
        def _():
            tell(onward)

    def send(copy):
        copy.start()

    def cross(d):
        return {"gx": lax.rem(chip + d, chips) * 2 + core}

    for d in range(1, gx):
        send(remote(ma.at[me_x], ma.at[me_x], ma_send, ma_recv,
                    {"gx": lax.rem(me_x + d, gx)}))
    for rel in (0, 1):
        send_own(0, rel)
    for v in (0, 1):
        for d in range(1, chips):
            ref, sem = a_piece(me_x, 0, 0, v)
            send(remote(ref, ref, a_sy.at[d], sem, cross(d)))
    for r in list(range(1, rows)) + [0]:
        send(remote(a_all.at[me_x, r], a_all.at[me_x, r], a_sp,
                    a_recv.at[me_x, r], {"gx": partner}))
    for q, rel in opening:
        send_own(q, rel)

    def prepare(g, r, v):
        at = pl.ds(v * half, half)
        values = jnp.concatenate([a_all[g, r, s, at] for s in range(slots)], axis=1)
        high = values.astype(jnp.bfloat16)
        a_hl[g, r, v * half:(v + 1) * half] = high
        low = (values - high.astype(jnp.float32)).astype(jnp.bfloat16)
        a_hl[g, r, tile + v * half:tile + (v + 1) * half] = low

    def unpack_one(src, q):
        value = jnp.zeros((tile, tile), jnp.float32)
        for b in range(blocks):
            packed = p_all[src, b, head + q * tile:head + (q + 1) * tile]
            code = p_all[src, b, :head]
            high = packed.astype(jnp.bfloat16).astype(jnp.float32)
            low = packed - high
            turn = lambda x: [x] + [pltpu.roll(x, s * width, 1) for s in range(1, CUTS)]
            highs, lows, codes = turn(high), turn(low), turn(code)
            for n in range(CUTS):
                t = b * CUTS + n
                if t >= tiles_p:
                    continue
                parts = [highs[-n % CUTS], highs[(1 - n) % CUTS],
                         lows[(2 - n) % CUTS], lows[(3 - n) % CUTS]]
                kinds = [codes[(p - n) % CUTS] for p in range(CUTS)]
                chosen, kind = parts[3], kinds[3]
                for p in (2, 1, 0):
                    chosen = jnp.where(group == p, parts[p], chosen)
                    kind = jnp.where(group8 == p, kinds[p], kind)
                want = (group8 % COLS_DEV).astype(jnp.float32)
                keep = jnp.where(kind == want, 1.0, 0.0)
                keep = jnp.concatenate([keep] * (tile // 8), axis=0)
                placed = jnp.where(keep > 0.5, chosen, 0.0)
                value = placed if t % slots_p == 0 else value + placed
                if t % slots_p == slots_p - 1:
                    side = q % 2 * tile
                    p_mul[q // 2, src * inner + t // slots_p, :, side:side + tile] = (
                        value.astype(jnp.bfloat16))

    def source(side, d):
        src = me_y - d if side == 0 else me_y + d
        return src, src >= 0 if side == 0 else src < gy

    def forward(q, d, rel):
        for side in (0, 1):
            src, there = source(side, d)

            @pl.when(jnp.logical_and(on_side(side, rel), jnp.logical_and(there, has_next[side])))
            def _(src=src, side=side):
                for b in range(blocks):
                    arrive(p_block(src, q, b), p_recv.at[src, q, b])
                    p_copy(side, src, q, b).start()

    def advance(n):
        for kind, q, d, rel in stages[n]:
            if kind == "own":
                send_own(q, rel)
            elif kind == "mid":
                send_own(q, rel, between)
            else:
                forward(q, d, rel)

    def unpack(q):
        for d in range(1, gy):
            for side in (0, 1):
                src, there = source(side, d)

                @pl.when(there)
                def _(src=src, side=side):
                    loose = q < straight and d == 2

                    @pl.when(True if loose else jnp.logical_not(has_next[side]))
                    def _():
                        for b in range(blocks):
                            arrive(p_block(src, q, b), p_recv.at[src, q, b])
                    unpack_one(src, q)

    def chip_at(d):
        return lax.rem(chip + d, chips)

    def relay_copies(r, o, v):
        copies = []
        for d in range(1, chips):
            came = lax.rem(chip - d + chips, chips)
            g = came * 2 + (core if r == 0 else o)
            ref, sem = a_piece(g, r, core, v)
            copies.append((ref, sem, remote(
                ref, ref, a_sf.at[d], sem, {"gx": partner})))
        return copies

    def relay(r, o, v):
        for ref, sem, copy in relay_copies(r, o, v):
            arrive(ref, sem)
            copy.start()

    lane_id = lax.broadcasted_iota(jnp.int32, (quarter, tile), 1)

    def product(g, r, v, cuts):
        picks = [sa[g, 0, r * slots + s] for s in range(slots)]
        first = cuts[0] % 2 * tile
        span = pl.ds(first, len(cuts) * tile)
        right = jnp.concatenate([p_mul[cuts[0] // 2, i, :, span] for i in picks], axis=0)
        if v is None:
            left, size = a_hl[g, r], tile
        else:
            left, size = jnp.concatenate(
                [a_hl[g, r, pl.ds(b + v * half, half)] for b in (0, tile)], axis=0), half
        out = jnp.dot(left, right, preferred_element_type=jnp.float32)
        results = []
        for n in range(len(cuts)):
            both = out[:size, n * tile:(n + 1) * tile] + out[size:, n * tile:(n + 1) * tile]
            both = both + pltpu.roll(both, half, 1)
            results.append(jnp.concatenate(
                [jnp.where(lane_id < half, both[b:b + quarter], both[b + quarter:b + half])
                 for b in range(0, size, half)], axis=0))
        return results

    def c_copy(z, i, q, v=None):
        at = pl.ds(0, half) if v is None else pl.ds(v * quarter, quarter)
        return remote(c_send.at[z, i, q, at], c_recv.at[me_z, i, q, at], c_ss.at[z],
                      c_rs.at[lax.rem(me_z - z - 1 + 2 * gz, gz), i, q // (CUTS - 1)], {"gz": z})

    def emit(spots, cuts):
        results = []
        for group_of in cuts:
            results += [(g, r, v, group_of, product(g, r, v, group_of)) for g, r, v in spots]
        for g, r, v, group_of, values in results:
            at = g * rows + r
            z, i = at // rows_out, lax.rem(at, rows_out)
            for q, value in zip(group_of, values):
                if v is None:
                    c_send[z, i, q] = value
                else:
                    c_send[z, i, q, v * quarter:(v + 1) * quarter] = value

            @pl.when(z != me_z)
            def _():
                for q in group_of:
                    c_copy(z, i, q, v).start()

    def near_row(n):
        return chip * 2 + n // rows, lax.rem(n, rows)

    def far_row(n):
        r = n // (2 * far)
        o = lax.rem(n // far, 2)
        return chip_at(1 + lax.rem(n, far)) * 2 + o, r

    n_near, n_far = 2 * rows, 2 * rows * far

    def near(q):
        emit([near_row(n) + (None,) for n in range(n_near)], ((q,),))

    def far_rows(r, sides, v, cuts):
        for d in range(1, chips):
            emit([(chip_at(d) * 2 + o, r, v) for o in sides], cuts)

    def prepare_far(r, sides, v):
        for d in range(1, chips):
            for o in sides:
                g = chip_at(d) * 2 + o
                for h in (0,) if r == 0 else (0, 1):
                    direct = core == (o if r == 0 else h)

                    @pl.when(jnp.logical_not(direct))
                    def _(g=g, h=h):
                        arrive(*a_piece(g, r, h, v))
                prepare(g, r, v)

    for r in range(rows):
        for v in (0, 1):
            prepare(me_x, r, v)
    if straight:
        @pl.when(between)
        def _():
            pl.semaphore_wait(far_ok, 1)
            tell(-onward)
    for r in list(range(1, rows)) + [0]:
        arrive(a_all.at[partner, r], a_recv.at[partner, r])
    for r in range(1, rows):
        for o in (0, 1):
            for v in (0, 1):
                for d in range(1, chips):
                    ref, sem = a_piece(chip * 2 + o, r, core, v)
                    send(remote(ref, ref, a_sy.at[d], sem, cross(d)))
    if straight:
        @pl.when(jnp.logical_not(between))
        def _():
            pl.semaphore_wait(far_ok, 1)
            for q in range(straight):
                for b in range(blocks):
                    ref = p_block(me_y, q, b)
                    remote(ref, ref, far_send, p_recv.at[me_y, q, b],
                           {"gy": gy - 1 - me_y}).start()
            send_own(CUTS - 1, 0)
    for q in range(CUTS):
        unpack_one(me_y, q)
    arrive(ma.at[pl.ds(0, gx - 1)], ma_recv)
    move = pltpu.make_async_copy(ma, sa, s_sem)
    move.start()
    for r in range(rows):
        for v in (0, 1):
            prepare(partner, r, v)
    move.wait()

    last_row = (rows - 1, 1)
    middle = [(r, o) for r in range(1, rows) for o in (0, 1) if (r, o) != last_row]
    both = (0, 1)
    near_mine = (chip * n_near) // rows_out == me_z

    def all_rows(n_more):
        total = n_near + n_more
        begin = jnp.where(near_mine, n_near, 0)
        spots = []
        for n in range(total):
            m = lax.rem(n + begin, total)
            is_near = m < n_near
            g0, r0 = near_row(m)
            g1, r1 = far_row(jnp.maximum(m - n_near, 0)) if far else (g0, r0)
            spots.append((jnp.where(is_near, g0, g1), jnp.where(is_near, r0, r1), None))
        return spots

    def sweep(spots, q):
        for n in range(0, len(spots), 3):
            emit(spots[n:n + 3], ((q,),))

    n_first = 2 * far
    advance(0)
    advance(1)
    relay(0, 0, 0)
    advance(2)
    advance(3)
    prepare_far(0, both, 0)
    relay(0, 0, 1)
    unpack(0)
    far_rows(0, both, 0, ((0,),))
    near(0)
    unpack(1)
    far_rows(0, both, 0, ((1,),))
    near(1)
    advance(4)
    prepare_far(0, both, 1)
    far_rows(0, both, 1, ((0, 1),))
    for r, o in middle:
        relay(r, o, 0)
    advance(5)
    for r, o in middle:
        relay(r, o, 1)
        prepare_far(r, (o,), 0)
        far_rows(r, (o,), 0, ((0, 1),))
    advance(6)
    for r, o in middle:
        prepare_far(r, (o,), 1)
        far_rows(r, (o,), 1, ((0, 1),))
    spots = all_rows(n_far - far if rows > 1 else n_far)
    soon, later = spots[:n_near], spots[n_near:]
    unpack(2)
    if rows > 1:
        relay(*last_row, 0)
    emit(soon, ((2,),))
    unpack(3)
    emit(soon, ((3,),))
    if rows > 1:
        prepare_far(rows - 1, (1,), 0)
        far_rows(rows - 1, (1,), 0, ((0, 1), (2, 3)))
        relay(*last_row, 1)
    emit(later, ((2, 3),))
    if rows > 1:
        prepare_far(rows - 1, (1,), 1)
        far_rows(rows - 1, (1,), 1, ((0, 1), (2, 3)))

    lanes = lax.broadcasted_iota(jnp.int32, (half, tile), 1)

    spot = lanes // width

    def finish(n, cuts, fresh):
        i = jnp.where(near_mine, n, n % (rows_out // rows) * rows + n // (rows_out // rows))
        top = [None, None]
        low = [None, None]
        for d in range(1, gz):
            z = lax.rem(me_z + d, gz)
            arrive(c_recv.at[z, i, pl.ds(cuts[0], len(cuts))], c_rs.at[d - 1, i, 0 if fresh else 1])
        for q in cuts:
            value = c_send[me_z, i, q]
            for d in range(1, gz):
                value = value + c_recv[lax.rem(me_z + d, gz), i, q]
            turned = [value] + [pltpu.roll(value, s * width, 1) for s in range(1, CUTS)]
            for c in range(COLS_DEV):
                for store, base in ((top, c), (low, c + COLS_DEV)):
                    piece = turned[(q - base) % CUTS]
                    old = store[c]
                    store[c] = piece if old is None else jnp.where(spot == q, piece, old)
        ours = spot >= cuts[0]
        for c in range(COLS_DEV):
            lane_to = slice(c * tile, (c + 1) * tile)
            for b in (0, 1):
                for e, store in enumerate((top, low)):
                    to = pl.ds(pl.multiple_of(i * tile + b * half + e * quarter, quarter), quarter)
                    at = slice(b * quarter, (b + 1) * quarter)
                    value = store[c][at]
                    if not fresh:
                        value = jnp.where(ours[at], value, o_ref[to, lane_to])
                    o_ref[to, lane_to] = value

    final = rows_out - 1
    for spans in (range(final), range(final, rows_out)):
        for n in spans:
            finish(n, range(CUTS - 1), True)
        for n in spans:
            finish(n, (CUTS - 1,), False)

    arrive(ma.at[pl.ds(0, gx - 1)], ma_send)
    for d in range(1, chips):
        arrive(a_all.at[me_x], a_sy.at[d])
        arrive(a_all.at[me_x], a_sf.at[d])
    arrive(a_all.at[me_x], a_sp)
    for side in (0, 1):
        for d in range(0, gy):
            src, there = source(side, d)

            @pl.when(jnp.logical_and(there, has_next[side]))
            def _(src=src, side=side, d=d):
                skip = head + straight * tile if straight and d == 2 else 0
                ref = p_all.at[src, :, pl.ds(skip, head + CUTS * tile - skip)]
                arrive(ref, p_send.at[side, src])
    if straight:
        @pl.when(jnp.logical_not(between))
        def _():
            arrive(p_all.at[me_y, :, pl.ds(0, head + straight * tile)], far_send)
    for d in range(1, gz):
        z = lax.rem(me_z + d, gz)
        arrive(c_send.at[z], c_ss.at[z])


def body(gx, gy, gz, a_vals, a_cols, a_count, p_vals, p_cols, p_count):
    if a_vals.shape[3] % 2:
        wide = [(0, 0)] * 3 + [(0, 1)]
        a_vals = jnp.pad(a_vals, wide + [(0, 0)] * 2)
        a_cols = jnp.pad(a_cols, wide)
    rows, slots, tile = a_vals.shape[1], a_vals.shape[3], a_vals.shape[-1]
    inner, slots_p = p_vals.shape[1], p_vals.shape[3]
    tiles_p = inner * slots_p
    blocks = -(-tiles_p // CUTS)
    rows_out = gx * rows // gz
    chips = max(gx // 2, 1)
    dma = pltpu.SemaphoreType.DMA
    any_spec = pl.BlockSpec(memory_space=pl.ANY)
    smem_spec = pl.BlockSpec(memory_space=pltpu.SMEM)
    return pl.pallas_call(
        functools.partial(kernel, gx, gy, gz, slots_p, tiles_p),
        out_shape=pltpu.VMEM((rows_out * tile, COLS_DEV * tile), jnp.float32),
        in_specs=[any_spec] * 2 + [smem_spec] * 4,
        out_specs=pl.BlockSpec(memory_space=pltpu.VMEM),
        scratch_shapes=[
            pltpu.VMEM((gx, rows, slots, tile, tile), jnp.float32),
            pltpu.VMEM((gx, rows, 2 * tile, slots * tile), jnp.bfloat16),
            pltpu.VMEM((tiles_p, tile, tile), jnp.float32),
            pltpu.VMEM((gy, blocks, 8 + CUTS * tile, tile), jnp.float32),
            pltpu.VMEM((gx, 8, 128), jnp.int32),
            pltpu.SMEM((gx, 8, 128), jnp.int32),
            pltpu.VMEM((CUTS // 2, gy * inner + 1, tile, 2 * tile), jnp.bfloat16),
            pltpu.VMEM((gz, rows_out, CUTS, tile // 2, tile), jnp.float32),
            pltpu.VMEM((gz, rows_out, CUTS, tile // 2, tile), jnp.float32),
            dma((gx, max(4 * rows - 2, rows))),
            dma((chips,)),
            dma,
            dma((chips,)),
            dma,
            dma((gy, CUTS, blocks)),
            dma((2, gy)),
            dma,
            dma,
            dma,
            dma((max(gz - 1, 1), rows_out, 2)),
            dma((gz,)),
            pltpu.SemaphoreType.REGULAR,
            dma,
        ],
        compiler_params=pltpu.CompilerParams(collective_id=0, has_side_effects=True),
    )(
        a_vals[0, :, 0], p_vals.reshape(tiles_p, tile, tile),
        a_cols, a_count.reshape(-1), p_cols.reshape(-1), p_count.reshape(-1),
    )


def solution(mesh):
    placed = (
        P("gy", "gx", "gz", None, None, None),
        P("gy", "gx", "gz", None),
        P("gy", "gx", "gz"),
        P("gz", "gy", "gx", None, None, None),
        P("gz", "gy", "gx", None),
        P("gz", "gy", "gx"),
    )
    sizes = (mesh.shape["gx"], mesh.shape["gy"], mesh.shape["gz"])
    return jax.shard_map(
        functools.partial(body, *sizes),
        mesh=mesh, in_specs=placed, out_specs=P(("gy", "gz"), "gx"), check_vma=False,
    )
```

```python
import functools

import jax
import jax.numpy as jnp
from jax import lax
from jax.experimental import pallas as pl
from jax.experimental.pallas import tpu as pltpu
from jax.sharding import PartitionSpec as P

COLS_DEV = 2
CUTS = 4
MESH = pl.DeviceIdType.MESH


def plan(gy):
    if gy == 4:
        opening = [(1, 0), (1, 1), (2, 1), (2, 0)]
        stages = [
            [("fwd", 0, 1, 1), ("fwd", 0, 1, 0)],
            [("fwd", 1, 1, 1), ("fwd", 1, 1, 0)],
            [("fwd", 2, 1, 0), ("fwd", 2, 1, 1), ("mid", 3, 0, 0), ("mid", 3, 0, 1)],
            [("fwd", 3, 1, 0)],
            [("fwd", 2, 2, 1)],
            [("fwd", 3, 1, 1)],
            [("fwd", 3, 2, 1)],
        ]
        return opening, stages, 2
    opening = [(q, rel) for q in range(1, CUTS) for rel in (0, 1)]
    waves = [[("fwd", q, d, rel) for d in range(1, gy) for rel in (0, 1)] for q in range(CUTS)]
    return opening, [[], [], waves[0], waves[1], waves[2], [], waves[3]], 0


def kernel(
    gx, gy, gz, slots_p, tiles_p,
    a_ref, p_ref, ac_ref, an_ref, pc_ref, pn_ref, o_ref,
    a_all, a_hl, p_own, p_all, ma, sa, p_mul, c_send, c_recv,
    a_recv, a_near, a_sy, a_sp, a_sf, p_load, p_recv, p_send,
    ma_recv, ma_send, s_sem, c_rs, c_ss, far_ok, far_send,
):
    rows, slots, tile = a_ref.shape[0], a_ref.shape[1], a_ref.shape[2]
    blocks = p_all.shape[1]
    head = 8
    inner = tiles_p // slots_p
    rows_out = gx * rows // gz
    zero_tile = gy * inner
    width = tile // CUTS
    half = tile // 2
    quarter = half // 2
    part = slots // 2
    opening, stages, straight = plan(gy)
    chips = gx // 2
    far = chips - 1
    me_x, me_y, me_z = lax.axis_index("gx"), lax.axis_index("gy"), lax.axis_index("gz")
    chip, core = me_x // 2, me_x % 2
    partner = chip * 2 + (1 - core)
    has_next = (me_y + 1 < gy, me_y >= 1)

    def remote(src, dst, send, recv, where):
        return pltpu.make_async_remote_copy(
            src_ref=src, dst_ref=dst, send_sem=send, recv_sem=recv,
            device_id=where, device_id_type=MESH)

    def arrive(ref, sem):
        pltpu.make_async_copy(ref, ref, sem).wait()

    barrier = pltpu.get_barrier_semaphore()
    for name, size, me in (("gx", gx, me_x), ("gz", gz, me_z)):
        for d in range(1, size):
            pl.semaphore_signal(
                barrier, inc=1, device_id={name: lax.rem(me + d, size)}, device_id_type=MESH
            )
    for side, step in ((0, 1), (1, -1)):
        @pl.when(has_next[side])
        def _(step=step):
            pl.semaphore_signal(
                barrier, inc=1, device_id={"gy": lax.rem(me_y + step + gy, gy)},
                device_id_type=MESH)

    load = pltpu.make_async_copy(p_ref, p_own, p_load)
    load.start()

    def a_piece(g, r, h, v, gap):
        at = pl.ds(v * half, half)
        spot = (gap - 1) * 2 + lax.rem(g, 2)
        if r == 0:
            return a_all.at[g, 0, :, at], a_recv.at[spot, v]
        return (a_all.at[g, r, pl.ds(h * part, part), at],
                a_recv.at[spot, 2 + (r - 1) * 4 + h * 2 + v])

    own_loads = [pltpu.make_async_copy(a_ref.at[r], a_all.at[me_x, r], a_near.at[0])
                 for r in range(rows)]
    for copy in own_loads:
        copy.start()

    line = lax.broadcasted_iota(jnp.int32, (8, 128), 0)
    lane = lax.broadcasted_iota(jnp.int32, (8, 128), 1)
    meta = jnp.zeros((8, 128), jnp.int32)
    for r in range(rows):
        for s in range(slots):
            pick = jnp.where(s < an_ref[r], ac_ref[0, r, 0, s], zero_tile)
            meta = jnp.where((line == 0) & (lane == r * slots + s), pick, meta)
    ma[me_x] = meta
    group = lax.broadcasted_iota(jnp.int32, (tile, tile), 1) // width
    group8 = lax.broadcasted_iota(jnp.int32, (8, tile), 1) // width
    for q in range(CUTS // 2):
        p_mul[q, zero_tile] = jnp.zeros_like(p_mul[q, zero_tile])

    load.wait()
    for b in range(blocks):
        mine = [b * CUTS + t for t in range(CUTS) if b * CUTS + t < tiles_p]
        code = jnp.full((8, tile), -1.0, jnp.float32)
        for n, t in enumerate(mine):
            kind = jnp.where(t % slots_p < pn_ref[t // slots_p], pc_ref[t], -1)
            code = jnp.where(group8 == n, kind.astype(jnp.float32), code)
        for q in range(CUTS):
            value = jnp.zeros((tile, tile), jnp.float32)
            for n, t in enumerate(mine):
                shift = (n - q) % CUTS * width
                turned = pltpu.roll(p_own[t], shift, 1) if shift else p_own[t]
                value = jnp.where(group == n, turned, value)
            p_all[me_y, b, head + q * tile:head + (q + 1) * tile] = value
        p_all[me_y, b, :head] = code
    arrive(a_all.at[me_x], a_near.at[0])

    neighbours = jnp.where(has_next[0], 1, 0) + jnp.where(has_next[1], 1, 0)
    pl.semaphore_wait(barrier, gx + gz - 2 + neighbours)

    def p_block(src, q, b):
        if q == 0:
            return p_all.at[src, b, pl.ds(0, head + tile)]
        return p_all.at[src, b, pl.ds(head + q * tile, tile)]

    def p_copy(side, src, q, b):
        ref = p_block(src, q, b)
        step = 1 if side == 0 else -1
        slot = gy if side == 0 and src is me_y else src
        return remote(ref, ref, p_send.at[slot], p_recv.at[src, q, b],
                      {"gy": lax.rem(me_y + step + gy, gy)})

    near_side = jnp.where(2 * me_y < gy - 1, 0, 1)

    def on_side(side, rel):
        return near_side == side if rel == 0 else near_side != side

    def send_own(q, rel, only=True):
        for side in (0, 1):
            @pl.when(jnp.logical_and(only, jnp.logical_and(on_side(side, rel), has_next[side])))
            def _(side=side):
                for b in range(blocks):
                    p_copy(side, me_y, q, b).start()

    between = jnp.logical_and(has_next[0], has_next[1])
    onward = jnp.where(near_side == 0, 1, -1)

    def tell(step):
        pl.semaphore_signal(far_ok, inc=1, device_id={"gy": me_y + step}, device_id_type=MESH)

    if straight:
        @pl.when(between)
        def _():
            tell(onward)

    def send(copy):
        copy.start()

    def cross(d):
        return {"gx": lax.rem(chip + d, chips) * 2 + core}

    for d in range(1, gx):
        send(remote(ma.at[me_x], ma.at[me_x], ma_send, ma_recv,
                    {"gx": lax.rem(me_x + d, gx)}))
    for rel in (0, 1):
        send_own(0, rel)
    for v in (0, 1):
        for d in range(1, chips):
            ref, sem = a_piece(me_x, 0, 0, v, chips - d)
            send(remote(ref, ref, a_sy.at[d - 1], sem, cross(d)))
    for r in list(range(1, rows)) + [0]:
        send(remote(a_all.at[me_x, r], a_all.at[me_x, r], a_sp,
                    a_near.at[1], {"gx": partner}))
    for q, rel in opening:
        send_own(q, rel)

    def prepare(g, r, v):
        at = pl.ds(v * half, half)
        values = jnp.concatenate([a_all[g, r, s, at] for s in range(slots)], axis=1)
        high = values.astype(jnp.bfloat16)
        a_hl[g, r, v * half:(v + 1) * half] = high
        low = (values - high.astype(jnp.float32)).astype(jnp.bfloat16)
        a_hl[g, r, tile + v * half:tile + (v + 1) * half] = low

    def unpack_one(src, q):
        value = jnp.zeros((tile, tile), jnp.float32)
        for b in range(blocks):
            packed = p_all[src, b, head + q * tile:head + (q + 1) * tile]
            code = p_all[src, b, :head]
            high = packed.astype(jnp.bfloat16).astype(jnp.float32)
            low = packed - high
            turn = lambda x: [x] + [pltpu.roll(x, s * width, 1) for s in range(1, CUTS)]
            highs, lows, codes = turn(high), turn(low), turn(code)
            for n in range(CUTS):
                t = b * CUTS + n
                if t >= tiles_p:
                    continue
                parts = [highs[-n % CUTS], highs[(1 - n) % CUTS],
                         lows[(2 - n) % CUTS], lows[(3 - n) % CUTS]]
                kinds = [codes[(p - n) % CUTS] for p in range(CUTS)]
                chosen, kind = parts[3], kinds[3]
                for p in (2, 1, 0):
                    chosen = jnp.where(group == p, parts[p], chosen)
                    kind = jnp.where(group8 == p, kinds[p], kind)
                want = (group8 % COLS_DEV).astype(jnp.float32)
                keep = jnp.where(kind == want, 1.0, 0.0)
                keep = jnp.concatenate([keep] * (tile // 8), axis=0)
                placed = jnp.where(keep > 0.5, chosen, 0.0)
                value = placed if t % slots_p == 0 else value + placed
                if t % slots_p == slots_p - 1:
                    side = q % 2 * tile
                    p_mul[q // 2, src * inner + t // slots_p, :, side:side + tile] = (
                        value.astype(jnp.bfloat16))

    def source(side, d):
        src = me_y - d if side == 0 else me_y + d
        return src, src >= 0 if side == 0 else src < gy

    def forward(q, d, rel):
        for side in (0, 1):
            src, there = source(side, d)

            @pl.when(jnp.logical_and(on_side(side, rel), jnp.logical_and(there, has_next[side])))
            def _(src=src, side=side):
                for b in range(blocks):
                    arrive(p_block(src, q, b), p_recv.at[src, q, b])
                    p_copy(side, src, q, b).start()

    def advance(n):
        for kind, q, d, rel in stages[n]:
            if kind == "own":
                send_own(q, rel)
            elif kind == "mid":
                send_own(q, rel, between)
            else:
                forward(q, d, rel)

    def unpack(q):
        for d in range(1, gy):
            for side in (0, 1):
                src, there = source(side, d)

                @pl.when(there)
                def _(src=src, side=side):
                    loose = q < straight and d == 2

                    @pl.when(True if loose else jnp.logical_not(has_next[side]))
                    def _():
                        for b in range(blocks):
                            arrive(p_block(src, q, b), p_recv.at[src, q, b])
                    unpack_one(src, q)

    def chip_at(d):
        return lax.rem(chip + d, chips)

    def relay_copies(r, o, v):
        copies = []
        for d in range(1, chips):
            came = lax.rem(chip - d + chips, chips)
            g = came * 2 + (core if r == 0 else o)
            ref, sem = a_piece(g, r, core, v, chips - d)
            copies.append((ref, sem, remote(
                ref, ref, a_sf.at[d - 1], sem, {"gx": partner})))
        return copies

    def relay(r, o, v):
        for ref, sem, copy in relay_copies(r, o, v):
            arrive(ref, sem)
            copy.start()

    lane_id = lax.broadcasted_iota(jnp.int32, (quarter, tile), 1)

    def product(g, r, v, cuts):
        picks = [sa[g, 0, r * slots + s] for s in range(slots)]
        first = cuts[0] % 2 * tile
        span = pl.ds(first, len(cuts) * tile)
        right = jnp.concatenate([p_mul[cuts[0] // 2, i, :, span] for i in picks], axis=0)
        if v is None:
            left, size = a_hl[g, r], tile
        else:
            left, size = jnp.concatenate(
                [a_hl[g, r, pl.ds(b + v * half, half)] for b in (0, tile)], axis=0), half
        out = jnp.dot(left, right, preferred_element_type=jnp.float32)
        results = []
        for n in range(len(cuts)):
            both = out[:size, n * tile:(n + 1) * tile] + out[size:, n * tile:(n + 1) * tile]
            both = both + pltpu.roll(both, half, 1)
            results.append(jnp.concatenate(
                [jnp.where(lane_id < half, both[b:b + quarter], both[b + quarter:b + half])
                 for b in range(0, size, half)], axis=0))
        return results

    def c_copy(z, i, q, v=None):
        at = pl.ds(0, half) if v is None else pl.ds(v * quarter, quarter)
        return remote(c_send.at[z, i, q, at], c_recv.at[me_z, i, q, at], c_ss.at[z],
                      c_rs.at[lax.rem(me_z - z - 1 + 2 * gz, gz), i, q // (CUTS - 1)], {"gz": z})

    def emit(spots, cuts):
        results = []
        for group_of in cuts:
            results += [(g, r, v, group_of, product(g, r, v, group_of)) for g, r, v in spots]
        for g, r, v, group_of, values in results:
            at = g * rows + r
            z, i = at // rows_out, lax.rem(at, rows_out)
            for q, value in zip(group_of, values):
                if v is None:
                    c_send[z, i, q] = value
                else:
                    c_send[z, i, q, v * quarter:(v + 1) * quarter] = value

            @pl.when(z != me_z)
            def _():
                for q in group_of:
                    c_copy(z, i, q, v).start()

    def near_row(n):
        return chip * 2 + n // rows, lax.rem(n, rows)

    def far_row(n):
        r = n // (2 * far)
        o = lax.rem(n // far, 2)
        return chip_at(1 + lax.rem(n, far)) * 2 + o, r

    n_near, n_far = 2 * rows, 2 * rows * far

    def near(q):
        emit([near_row(n) + (None,) for n in range(n_near)], ((q,),))

    def far_rows(r, sides, v, cuts):
        for d in range(1, chips):
            emit([(chip_at(d) * 2 + o, r, v) for o in sides], cuts)

    def prepare_far(r, sides, v):
        for d in range(1, chips):
            for o in sides:
                g = chip_at(d) * 2 + o
                for h in (0,) if r == 0 else (0, 1):
                    direct = core == (o if r == 0 else h)

                    @pl.when(jnp.logical_not(direct))
                    def _(g=g, h=h, d=d):
                        arrive(*a_piece(g, r, h, v, d))
                prepare(g, r, v)

    for r in range(rows):
        for v in (0, 1):
            prepare(me_x, r, v)
    if straight:
        @pl.when(between)
        def _():
            pl.semaphore_wait(far_ok, 1)
            tell(-onward)
    arrive(a_all.at[partner], a_near.at[1])
    for r in range(1, rows):
        for o in (0, 1):
            for v in (0, 1):
                for d in range(1, chips):
                    ref, sem = a_piece(chip * 2 + o, r, core, v, chips - d)
                    send(remote(ref, ref, a_sy.at[d - 1], sem, cross(d)))
    if straight:
        @pl.when(jnp.logical_not(between))
        def _():
            pl.semaphore_wait(far_ok, 1)
            for q in range(straight):
                for b in range(blocks):
                    ref = p_block(me_y, q, b)
                    remote(ref, ref, far_send, p_recv.at[me_y, q, b],
                           {"gy": gy - 1 - me_y}).start()
            send_own(CUTS - 1, 0)
    for q in range(CUTS):
        unpack_one(me_y, q)
    arrive(ma.at[pl.ds(0, gx - 1)], ma_recv)
    move = pltpu.make_async_copy(ma, sa, s_sem)
    move.start()
    for r in range(rows):
        for v in (0, 1):
            prepare(partner, r, v)
    move.wait()

    last_row = (rows - 1, 1)
    middle = [(r, o) for r in range(1, rows) for o in (0, 1) if (r, o) != last_row]
    both = (0, 1)
    near_mine = (chip * n_near) // rows_out == me_z

    def all_rows(n_more):
        total = n_near + n_more
        begin = jnp.where(near_mine, n_near, 0)
        spots = []
        for n in range(total):
            m = lax.rem(n + begin, total)
            is_near = m < n_near
            g0, r0 = near_row(m)
            g1, r1 = far_row(jnp.maximum(m - n_near, 0)) if far else (g0, r0)
            spots.append((jnp.where(is_near, g0, g1), jnp.where(is_near, r0, r1), None))
        return spots

    def sweep(spots, q):
        for n in range(0, len(spots), 3):
            emit(spots[n:n + 3], ((q,),))

    n_first = 2 * far
    advance(0)
    advance(1)
    relay(0, 0, 0)
    advance(2)
    advance(3)
    prepare_far(0, both, 0)
    relay(0, 0, 1)
    unpack(0)
    far_rows(0, both, 0, ((0,),))
    near(0)
    unpack(1)
    far_rows(0, both, 0, ((1,),))
    near(1)
    advance(4)
    prepare_far(0, both, 1)
    far_rows(0, both, 1, ((0, 1),))
    for r, o in middle:
        relay(r, o, 0)
    advance(5)
    for r, o in middle:
        relay(r, o, 1)
        prepare_far(r, (o,), 0)
        far_rows(r, (o,), 0, ((0, 1),))
    advance(6)
    for r, o in middle:
        prepare_far(r, (o,), 1)
        far_rows(r, (o,), 1, ((0, 1),))
    spots = all_rows(n_far - far if rows > 1 else n_far)
    soon, later = spots[:n_near], spots[n_near:]
    unpack(2)
    if rows > 1:
        relay(*last_row, 0)
    emit(soon, ((2,),))
    unpack(3)
    emit(soon, ((3,),))
    if rows > 1:
        prepare_far(rows - 1, (1,), 0)
        far_rows(rows - 1, (1,), 0, ((0, 1), (2, 3)))
        relay(*last_row, 1)
    emit(later, ((2, 3),))
    if rows > 1:
        prepare_far(rows - 1, (1,), 1)
        far_rows(rows - 1, (1,), 1, ((0, 1), (2, 3)))

    lanes = lax.broadcasted_iota(jnp.int32, (half, tile), 1)

    spot = lanes // width

    def finish(n, cuts, fresh):
        i = jnp.where(near_mine, n, n % (rows_out // rows) * rows + n // (rows_out // rows))
        top = [None, None]
        low = [None, None]
        for d in range(1, gz):
            z = lax.rem(me_z + d, gz)
            arrive(c_recv.at[z, i, pl.ds(cuts[0], len(cuts))], c_rs.at[d - 1, i, 0 if fresh else 1])
        for q in cuts:
            value = c_send[me_z, i, q]
            for d in range(1, gz):
                value = value + c_recv[lax.rem(me_z + d, gz), i, q]
            turned = [value] + [pltpu.roll(value, s * width, 1) for s in range(1, CUTS)]
            for c in range(COLS_DEV):
                for store, base in ((top, c), (low, c + COLS_DEV)):
                    piece = turned[(q - base) % CUTS]
                    old = store[c]
                    store[c] = piece if old is None else jnp.where(spot == q, piece, old)
        ours = spot >= cuts[0]
        for c in range(COLS_DEV):
            lane_to = slice(c * tile, (c + 1) * tile)
            for b in (0, 1):
                for e, store in enumerate((top, low)):
                    to = pl.ds(pl.multiple_of(i * tile + b * half + e * quarter, quarter), quarter)
                    at = slice(b * quarter, (b + 1) * quarter)
                    value = store[c][at]
                    if not fresh:
                        value = jnp.where(ours[at], value, o_ref[to, lane_to])
                    o_ref[to, lane_to] = value

    final = rows_out - 1
    for spans in (range(final), range(final, rows_out)):
        for n in spans:
            finish(n, range(CUTS - 1), True)
        for n in spans:
            finish(n, (CUTS - 1,), False)

    arrive(ma.at[pl.ds(0, gx - 1)], ma_send)
    for d in range(1, chips):
        arrive(a_all.at[me_x], a_sy.at[d - 1])
        arrive(a_all.at[me_x], a_sf.at[d - 1])
    arrive(a_all.at[me_x], a_sp)
    for side in (0, 1):
        for d in range(0, gy):
            src, there = source(side, d)

            @pl.when(jnp.logical_and(there, has_next[side]))
            def _(src=src, side=side, d=d):
                skip = head + straight * tile if straight and d == 2 else 0
                ref = p_all.at[src, :, pl.ds(skip, head + CUTS * tile - skip)]
                arrive(ref, p_send.at[gy if side == 0 and d == 0 else src])
    if straight:
        @pl.when(jnp.logical_not(between))
        def _():
            arrive(p_all.at[me_y, :, pl.ds(0, head + straight * tile)], far_send)
    for d in range(1, gz):
        z = lax.rem(me_z + d, gz)
        arrive(c_send.at[z], c_ss.at[z])


def body(gx, gy, gz, a_vals, a_cols, a_count, p_vals, p_cols, p_count):
    if a_vals.shape[3] % 2:
        wide = [(0, 0)] * 3 + [(0, 1)]
        a_vals = jnp.pad(a_vals, wide + [(0, 0)] * 2)
        a_cols = jnp.pad(a_cols, wide)
    rows, slots, tile = a_vals.shape[1], a_vals.shape[3], a_vals.shape[-1]
    inner, slots_p = p_vals.shape[1], p_vals.shape[3]
    tiles_p = inner * slots_p
    blocks = -(-tiles_p // CUTS)
    rows_out = gx * rows // gz
    chips = max(gx // 2, 1)
    dma = pltpu.SemaphoreType.DMA
    any_spec = pl.BlockSpec(memory_space=pl.ANY)
    smem_spec = pl.BlockSpec(memory_space=pltpu.SMEM)
    return pl.pallas_call(
        functools.partial(kernel, gx, gy, gz, slots_p, tiles_p),
        out_shape=pltpu.VMEM((rows_out * tile, COLS_DEV * tile), jnp.float32),
        in_specs=[any_spec] * 2 + [smem_spec] * 4,
        out_specs=pl.BlockSpec(memory_space=pltpu.VMEM),
        scratch_shapes=[
            pltpu.VMEM((gx, rows, slots, tile, tile), jnp.float32),
            pltpu.VMEM((gx, rows, 2 * tile, slots * tile), jnp.bfloat16),
            pltpu.VMEM((tiles_p, tile, tile), jnp.float32),
            pltpu.VMEM((gy, blocks, 8 + CUTS * tile, tile), jnp.float32),
            pltpu.VMEM((gx, 8, 128), jnp.int32),
            pltpu.SMEM((gx, 8, 128), jnp.int32),
            pltpu.VMEM((CUTS // 2, gy * inner + 1, tile, 2 * tile), jnp.bfloat16),
            pltpu.VMEM((gz, rows_out, CUTS, tile // 2, tile), jnp.float32),
            pltpu.VMEM((gz, rows_out, CUTS, tile // 2, tile), jnp.float32),
            dma((max(2 * chips - 2, 1), max(4 * rows - 2, 2))),
            dma((2,)),
            dma((max(chips - 1, 1),)),
            dma,
            dma((max(chips - 1, 1),)),
            dma,
            dma((gy, CUTS, blocks)),
            dma((gy + 1,)),
            dma,
            dma,
            dma,
            dma((max(gz - 1, 1), rows_out, 2)),
            dma((gz,)),
            pltpu.SemaphoreType.REGULAR,
            dma,
        ],
        compiler_params=pltpu.CompilerParams(collective_id=0, has_side_effects=True),
    )(
        a_vals[0, :, 0], p_vals.reshape(tiles_p, tile, tile),
        a_cols, a_count.reshape(-1), p_cols.reshape(-1), p_count.reshape(-1),
    )


def solution(mesh):
    placed = (
        P("gy", "gx", "gz", None, None, None),
        P("gy", "gx", "gz", None),
        P("gy", "gx", "gz"),
        P("gz", "gy", "gx", None, None, None),
        P("gz", "gy", "gx", None),
        P("gz", "gy", "gx"),
    )
    sizes = (mesh.shape["gx"], mesh.shape["gy"], mesh.shape["gz"])
    return jax.shard_map(
        functools.partial(body, *sizes),
        mesh=mesh, in_specs=placed, out_specs=P(("gy", "gz"), "gx"), check_vma=False,
    )
```
